32 devices in a mesh: gx: 4 (over z), gy: 4 (over x, core), gz: 2 (over y).
Axes of the slice: x: 2, y: 2, z: 4, core: 2. Of those that a mesh axis runs over, the one named last changes fastest.
Arguments:
- density: float32 [16, 128, 256], P('gx', 'gy', 'gz'), may hold values from 0.6 to 1.4
- velocity: float32 [3, 16, 128, 256], P(None, 'gx', 'gy', 'gz'), may hold values from -0.3 to 0.3
- solid_mask: int32 [16, 128, 256], P('gx', 'gy', 'gz'), may hold values 0 or 1
Outputs:
- density_final: float32 [16, 128, 256], P('gx', 'gy', 'gz')
- momentum: float32 [3, 16, 128, 256], P(None, 'gx', 'gy', 'gz')
The draws below stay inside these ranges and needn't reach their ends.
All inputs are finite; a program needn't handle non-finite values.
Results may differ from the reference program's by a relative error of at most 0.0003.
Values sent between devices are 32-bit elements.
A program may use at most 64 MiB of HBM per device.

```python
import jax
import jax.numpy as jnp
import numpy as np
from jax import lax

ITERS = 4
NX = 16
NY = 128
NZ = 256


def set_ends(result, key, low, largest):
    shape = result.shape
    place = [jax.random.randint(jax.random.fold_in(key, axis), (), 0, shape[axis]) for axis in range(len(shape))]
    result = result.at[tuple(place)].set(low)
    longest = shape.index(max(shape))
    place[longest] = (place[longest] + 1) % shape[longest]
    return result.at[tuple(place)].set(largest)


def block_levels(stream_key, dims, cuts, low, top_value):
    gain = 1.0
    for dim, shards_of in cuts:
        steps = jax.random.uniform(jax.random.fold_in(jax.random.fold_in(stream_key, 6), dim), (shards_of,), jnp.float32, low / len(cuts), top_value / len(cuts))
        gain = gain * jnp.repeat(jnp.exp(steps), dims[dim] // shards_of).reshape((-1,) + (1,) * (len(dims) - 1 - dim))
    return gain


def centred(key, dims, spread, most, shards=(), kind=jnp.bfloat16):
    result = spread * jax.random.normal(key, dims, jnp.float32)
    if shards:
        result = result * block_levels(key, dims, shards, -0.22, 0.18)
    return jnp.clip(result, -most, most).astype(kind)


def setup_inputs(seed: int = 0) -> dict:
    arg_keys = jax.random.split(jax.random.key(seed), 4)
    return {
        "density": jnp.clip(0.6 + 0.79999995 * jax.random.uniform(arg_keys[0], (NX, NY, NZ), jnp.float32) ** block_levels(arg_keys[0], (NX, NY, NZ), ((0, 4), (1, 4), (2, 2)), -0.2, 0.2), 0.6, 1.4),
        "velocity": centred(arg_keys[1], (3, NX, NY, NZ), 0.1, 0.3, ((1, 4), (2, 4), (3, 2)), jnp.float32),
        "solid_mask": set_ends((jax.random.randint(arg_keys[2], (NX, NY, NZ), 0, 10) < 1).astype(jnp.int32), jax.random.fold_in(arg_keys[2], 1), 0, 1),
    }


VELOCITIES = [(0, 0, 0), (1, 0, 0), (-1, 0, 0), (0, 1, 0), (0, -1, 0), (0, 0, 1), (0, 0, -1),
              (1, 1, 0), (-1, -1, 0), (1, -1, 0), (-1, 1, 0), (1, 0, 1), (-1, 0, -1),
              (1, 0, -1), (-1, 0, 1), (0, 1, 1), (0, -1, -1), (0, 1, -1), (0, -1, 1)]
WEIGHTS = [1.0 / 3.0] + [1.0 / 18.0] * 6 + [1.0 / 36.0] * 12
OPPOSITE = [0, 2, 1, 4, 3, 6, 5, 8, 7, 10, 9, 12, 11, 14, 13, 16, 15, 18, 17]
RELAX_RATE = 1.25


def equilibrium(density_now, velocity_now):
    velocity_table = jnp.asarray(np.array(VELOCITIES), jnp.float32)
    projected = jnp.tensordot(velocity_table, velocity_now, axes=1, precision=lax.Precision.HIGHEST)
    speed_sq = jnp.sum(velocity_now * velocity_now, axis=0)
    weights = jnp.asarray(np.array(WEIGHTS), jnp.float32).reshape((19, 1, 1, 1))
    return weights * density_now * (1.0 + 3.0 * projected + 4.5 * projected * projected - 1.5 * speed_sq)


def moments(fields):
    velocity_table = jnp.asarray(np.array(VELOCITIES), jnp.float32)
    density_now = jnp.sum(fields, axis=0)
    momentum_now = jnp.tensordot(velocity_table.T, fields, axes=1, precision=lax.Precision.HIGHEST)
    return density_now, momentum_now


def collide(fields, solid_mask):
    density_now, momentum_now = moments(fields)
    balance = equilibrium(density_now, momentum_now / density_now)
    relaxed = fields - RELAX_RATE * (fields - balance)
    bounced = fields[np.array(OPPOSITE)]
    return jnp.where(solid_mask[None] == 1, bounced, relaxed)


def reference(density, velocity, solid_mask):
    fields = equilibrium(density, velocity)
    for iteration in range(ITERS):
        collided = collide(fields, solid_mask)
        fields = jnp.stack([jnp.roll(collided[which_pop], VELOCITIES[which_pop], axis=(0, 1, 2))
                            for which_pop in range(19)])
    density_final, momentum = moments(fields)
    return density_final, momentum
```

```python
import functools

import jax
import jax.numpy as jnp
from jax import lax
from jax.experimental import pallas as pl
from jax.experimental.pallas import tpu as pltpu
from jax.sharding import PartitionSpec as P

ITERS = 4
RELAX_RATE = 1.25
AXES = ("gx", "gy", "gz")
MESH = pl.DeviceIdType.MESH
PAD = 8

CX = [(0, 0), (1, 0), (-1, 0), (0, 1), (0, -1)]
VEL = (
    [(1, a, b) for a, b in CX]
    + [(-1, a, b) for a, b in CX]
    + [(0, 1, 0), (0, 1, 1), (0, 1, -1)]
    + [(0, -1, 0), (0, -1, 1), (0, -1, -1)]
    + [(0, 0, 1), (0, 0, -1), (0, 0, 0)]
)
INDEX = {v: q for q, v in enumerate(VEL)}
NQ = len(VEL)


def neg(v):
    return tuple(-a for a in v)


OPP = [INDEX[neg(v)] for v in VEL]
WEIGHT = [{0: 1.0 / 3.0, 1: 1.0 / 18.0, 2: 1.0 / 36.0}[sum(abs(a) for a in v)] for v in VEL]
HALF = [q for q in range(NQ) if VEL[q] > (0, 0, 0)]
ZPOPS = {cz: [q for q in range(NQ) if VEL[q][2] == cz] for cz in (1, -1)}
ZSLOT = {1: 0, -1: 1}
EDGE_XZ = [(1, 0, 1), (1, 0, -1), (-1, 0, 1), (-1, 0, -1)]


def direction_sum(v, parts):
    total = None
    for a, part in zip(v, parts):
        if a:
            if total is None:
                total = part if a > 0 else -part
            else:
                total = total + part if a > 0 else total - part
    return total


def moments(f):
    pair_sum = {q: f[q] + f[OPP[q]] for q in HALF}
    pair_dif = {q: f[q] - f[OPP[q]] for q in HALF}
    rest = f[INDEX[(0, 0, 0)]]
    density = rest
    for q in HALF:
        density = density + pair_sum[q]
    momentum = []
    for axis in range(3):
        total = None
        for q in HALF:
            a = VEL[q][axis]
            if a:
                term = pair_dif[q]
                if total is None:
                    total = term if a > 0 else -term
                else:
                    total = total + term if a > 0 else total - term
        momentum.append(total)
    return density, momentum


def equilibrium(density, velocity, scale):
    ux, uy, uz = velocity
    base = 1.0 - 1.5 * (ux * ux + uy * uy + uz * uz)
    scaled = {w: (w * scale) * density for w in set(WEIGHT)}
    out = [None] * NQ
    out[INDEX[(0, 0, 0)]] = scaled[WEIGHT[INDEX[(0, 0, 0)]]] * base
    for q in HALF:
        along = direction_sum(VEL[q], velocity)
        even = base + 4.5 * along * along
        odd = 3.0 * along
        out[q] = scaled[WEIGHT[q]] * (even + odd)
        out[OPP[q]] = scaled[WEIGHT[q]] * (even - odd)
    return out


def collide(f, solid):
    density, momentum = moments(f)
    inverse = 1.0 / density
    balance = equilibrium(density, [m * inverse for m in momentum], RELAX_RATE)
    return [
        jnp.where(solid, f[OPP[q]], (1.0 - RELAX_RATE) * f[q] + balance[q]) for q in range(NQ)
    ]


def kernel(sizes, density, velocity, mask, density_out, momentum_out, grid, zsend, zrecv, esend, erecv, send_sem, recv_sem):
    nx, ny, nz = density.shape
    here = [lax.axis_index(a) for a in AXES]
    lane = lax.broadcasted_iota(jnp.int32, (ny, nz), 1)
    lane8 = lax.broadcasted_iota(jnp.int32, (PAD, nz), 1)
    moving = [v for v in VEL if v != (0, 0, 0)]

    def target(v):
        return tuple(
            lax.rem(here[a] + (v[a] + sizes[a]), sizes[a]) if v[a] else here[a] for a in range(3)
        )

    barrier = pltpu.get_barrier_semaphore()
    for v in moving:
        pl.semaphore_signal(barrier, inc=1, device_id=target(v), device_id_type=MESH)

    def refs(step, v):
        cx, cy, cz = v
        plane_src = nx if cx > 0 else 1
        plane_dst = 0 if cx > 0 else nx + 1
        row_src = ny if cy > 0 else PAD
        row_dst = 0 if cy > 0 else PAD + ny
        g = grid.at[step]
        if cx and not cy and not cz:
            first = 0 if cx > 0 else 5
            rows = pl.ds(PAD, ny)
            return (g.at[pl.ds(first, 5), plane_src, rows], g.at[pl.ds(first, 5), plane_dst, rows])
        if cx and cy:
            q = INDEX[v]
            return (g.at[q, plane_src, pl.ds(row_src, PAD)], g.at[q, plane_dst, pl.ds(row_dst, PAD)])
        if cx and cz:
            e = EDGE_XZ.index(v)
            return (esend.at[step, e], erecv.at[step, e])
        if cy and not cz:
            return None
        if cz and not cy:
            return (zsend.at[step, ZSLOT[cz]], zrecv.at[step, ZSLOT[cz], pl.ds(PAD, ny)])
        return (
            zsend.at[step, ZSLOT[cz], pl.ds(row_src - PAD, PAD) if cy < 0 else pl.ds(ny - PAD, PAD)],
            zrecv.at[step, ZSLOT[cz], pl.ds(row_dst, PAD)],
        )

    def copies(step, v):
        cx, cy, cz = v
        if cy and not cx and not cz:
            row_src = ny if cy > 0 else PAD
            row_dst = 0 if cy > 0 else PAD + ny
            g = grid.at[step]
            first = INDEX[(0, cy, 0)]
            inner = pl.ds(1, nx)
            pairs = [(g.at[pl.ds(first, 3), inner, pl.ds(row_src, PAD)], g.at[pl.ds(first, 3), inner, pl.ds(row_dst, PAD)])]
            for x in (1, -1):
                q = INDEX[(x, cy, 0)]
                pairs.append((g.at[q, inner, pl.ds(row_src, PAD)], g.at[q, inner, pl.ds(row_dst, PAD)]))
        else:
            pairs = [refs(step, v)]
        base = INDEX[v]
        slots = [base]
        if len(pairs) == 3:
            extra = NQ if cy > 0 else NQ + 2
            slots += [extra, extra + 1]
        return [
            pltpu.make_async_remote_copy(
                src_ref=src,
                dst_ref=dst,
                send_sem=send_sem.at[step, slot],
                recv_sem=recv_sem.at[step, slot],
                device_id=target(v),
                device_id_type=MESH,
            )
            for (src, dst), slot in zip(pairs, slots)
        ]

    def load(step, x):
        out = []
        for q, (cx, cy, cz) in enumerate(VEL):
            plane = x - cx + 1
            rows = pl.ds(PAD - cy, ny)
            value = grid[step, q, plane, rows, :]
            if cz:
                end = 0 if cz > 0 else nz - 1
                value = pltpu.roll(value, cz % nz, 1)
                if 1 <= plane <= nx:
                    item = ZPOPS[cz].index(q) * nx + plane - 1
                    column = zrecv[step, ZSLOT[cz], rows, :]
                    if item != end:
                        column = pltpu.roll(column, (end - item) % nz, 1)
                else:
                    tile = erecv[step, EDGE_XZ.index((cx, cy, cz))]
                    column = jnp.concatenate(
                        [tile if t == end else pltpu.roll(tile, (end - t) % nz, 1) for t in range(ny // PAD)],
                        axis=0,
                    )
                value = jnp.where(lane == end, column, value)
            out.append(value)
        return out

    def store(step, x, g, packs):
        for q in range(NQ):
            grid[step, q, x + 1, pl.ds(PAD, ny), :] = g[q]
        for cz in (1, -1):
            end = nz - 1 if cz > 0 else 0
            for i, q in enumerate(ZPOPS[cz]):
                item = i * nx + x
                moved = g[q] if item == end else pltpu.roll(g[q], (item - end) % nz, 1)
                packs[cz] = moved if packs[cz] is None else jnp.where(lane == item, moved, packs[cz])
                v = VEL[q]
                if (v[0] == 1 and x == nx - 1) or (v[0] == -1 and x == 0):
                    tile = None
                    for t in range(ny // PAD):
                        part = g[q][t * PAD:(t + 1) * PAD]
                        part = part if t == end else pltpu.roll(part, (t - end) % nz, 1)
                        tile = part if tile is None else jnp.where(lane8 == t, part, tile)
                    esend[step, EDGE_XZ.index(v)] = tile

    inner = list(range(1, nx - 1))
    outer = [0, nx - 1] if nx > 1 else [0]
    with_x = [v for v in moving if v[0]]
    without_x = [v for v in moving if not v[0]]
    sent = []

    def run(step, vs):
        for v in vs:
            for copy in copies(step, v):
                copy.start()
                sent.append(copy)

    def arrive(step, vs):
        for v in vs:
            for copy in copies(step, v):
                copy.wait_recv()

    for step in range(ITERS):
        packs = {1: None, -1: None}
        for x in inner + outer:
            if step == 0:
                f = equilibrium(density[x], [velocity[a, x] for a in range(3)], 1.0)
            else:
                if inner and x == inner[0] or not inner and x == 0:
                    arrive(step - 1, without_x)
                if x == 0:
                    arrive(step - 1, with_x)
                f = load(step - 1, x)
            store(step, x, collide(f, mask[x] == 1), packs)
        for cz in (1, -1):
            zsend[step, ZSLOT[cz]] = packs[cz]
        if step == 0:
            pl.semaphore_wait(barrier, len(moving))
        run(step, with_x + without_x)
    arrive(ITERS - 1, without_x)
    for x in inner + outer:
        if x == 0:
            arrive(ITERS - 1, with_x)
        total, momentum = moments(load(ITERS - 1, x))
        density_out[x] = total
        for a in range(3):
            momentum_out[a, x] = momentum[a]
    for copy in sent:
        copy.wait_send()


def local(sizes, density, velocity, solid_mask):
    nx, ny, nz = density.shape
    f32 = jnp.float32
    vmem = pl.BlockSpec(memory_space=pltpu.VMEM)
    return pl.pallas_call(
        functools.partial(kernel, sizes),
        out_shape=(
            jax.ShapeDtypeStruct(density.shape, f32),
            jax.ShapeDtypeStruct(velocity.shape, f32),
        ),
        in_specs=[vmem] * 3,
        out_specs=(vmem, vmem),
        scratch_shapes=[
            pltpu.VMEM((ITERS, NQ, nx + 2, ny + 2 * PAD, nz), f32),
            pltpu.VMEM((ITERS, 2, ny, nz), f32),
            pltpu.VMEM((ITERS, 2, ny + 2 * PAD, nz), f32),
            pltpu.VMEM((ITERS, 4, PAD, nz), f32),
            pltpu.VMEM((ITERS, 4, PAD, nz), f32),
            pltpu.SemaphoreType.DMA((ITERS, NQ + 4)),
            pltpu.SemaphoreType.DMA((ITERS, NQ + 4)),
        ],
        compiler_params=pltpu.CompilerParams(
            collective_id=0, has_side_effects=True, vmem_limit_bytes=40 * 1024 * 1024
        ),
    )(density, velocity, solid_mask)


def solution(mesh):
    sizes = [mesh.shape[a] for a in AXES]
    placed = (P("gx", "gy", "gz"), P(None, "gx", "gy", "gz"), P("gx", "gy", "gz"))
    return jax.shard_map(
        functools.partial(local, sizes),
        mesh=mesh,
        in_specs=placed,
        out_specs=(P("gx", "gy", "gz"), P(None, "gx", "gy", "gz")),
        check_vma=False,
    )
```
